32 devices in a mesh: lon: 4 (over z), lat: 4 (over y, x), dest: 2 (over core).
Axes of the slice: x: 2, y: 2, z: 4, core: 2. Of those that a mesh axis runs over, the one named last changes fastest.
Arguments:
- start_visits: bfloat16 [16, 16, 256, 256], P('lon', 'lat', None, 'dest'), may hold values from -6 to 6
- tiles: bfloat16 [16, 16, 4, 256, 256], P('lon', 'lat'), may hold values from -0.1875 to 0.1875
- codes: int32 [16, 16, 4], P('lon', 'lat'), may hold values from 0 to 8, as said below
- counts: int32 [16, 16], P('lon', 'lat'), may hold values from 1 to 4
- demo_nodes: int32 [4, 4, 1024], P('lon', 'lat', 'dest'), may hold values from 0 to 4095
Outputs:
- visits: bfloat16 [16, 16, 256, 256], P('lon', 'lat', None, 'dest')
- reward_grad: float32 [16, 16, 256], P('lon', 'lat')
The draws below stay inside these ranges and needn't reach their ends.
Inputs may be any that keep to these rules, and one draw needn't show every extreme that they name: `codes`: within one cluster the used slots name different source clusters.
All inputs are finite; a program needn't handle non-finite values.
Results may differ from the reference program's by a relative error of at most 0.0064.
Values may be sent and summed in bfloat16 or wider, within the bound.
No kernel may reach another device: no remote copies, remote signals or barrier semaphores. Data moves between devices by JAX's collectives and lax.ppermute only.
A program may use at most 64 MiB of HBM per device.

```python
import math
import jax
import jax.numpy as jnp
import numpy as np
from jax import lax

NODES = 256
DESTG = 128
SLOTS = 4
STEPS = 4
CLON = 4
CLAT = 4
DEMO = 512
NXC = 16
NYC = 16
DESTS = 256
N_LON = 4
N_LAT = 4
N_DEST = 2


def draw_codes(key, part):
    scores = jax.random.randint(key, (NXC, NYC, 9), 0, 1 << 20)
    scores = scores * 16 + jnp.arange(9, dtype=jnp.int32)
    order = jnp.argsort(scores, axis=-1, stable=True)
    return order[..., :SLOTS].astype(jnp.int32)


def place_ends(array, rng, smallest, largest):
    place = [jax.random.randint(jax.random.fold_in(rng, axis), (), 0, length) for axis, length in enumerate(array.shape)]
    longest = array.shape.index(max(array.shape))
    neighbour = place[:longest] + [(place[longest] + 1) % array.shape[longest]] + place[longest + 1:]
    return array.at[tuple(place)].set(smallest).at[tuple(neighbour)].set(largest)


def block_scale(own_key, shape, split, low, top_value):
    level = 1.0
    for dim, shards_of in split:
        draws = jax.random.uniform(jax.random.fold_in(jax.random.fold_in(own_key, 6), dim), (shards_of,), jnp.float32, low / len(split), top_value / len(split))
        level = level * jnp.repeat(jnp.exp(draws), shape[dim] // shards_of).reshape((-1,) + (1,) * (len(shape) - 1 - dim))
    return level


def rank_bounds(number_of, lean):
    portions = [(1 << 20) // math.isqrt(standing ** lean) + 1 for standing in range(1, number_of + 1)]
    spread = 1 + sum(portions) // (1 << 30)
    return np.cumsum(np.array([max(1, weight // spread) for weight in portions]))


def ranked(key, shape, number_of, skew):
    listing = rank_bounds(number_of, skew)
    pick = jax.random.randint(jax.random.fold_in(key, 1), shape, 0, int(listing[number_of - 1]))
    rank = jnp.searchsorted(jnp.asarray(listing, jnp.int32), pick, side="right")
    return jax.random.permutation(jax.random.fold_in(key, 2), number_of)[rank].astype(jnp.int32)


def gaussian(own_key, dims, deviation, most, split=(), kind=jnp.bfloat16):
    factor_of = block_scale(own_key, dims, split, -0.22, 0.18) if split else 1.0
    values = jax.random.normal(own_key, dims, jnp.float32) * deviation * factor_of
    return jnp.minimum(jnp.maximum(values, -most), most).astype(kind)


def setup_inputs(seed: int = 0) -> dict:
    splits = jax.random.split(jax.random.key(seed), 6)
    start_visits = gaussian(splits[0], (NXC, NYC, NODES, DESTS), 1.0, 6.0, ((0, 4), (1, 4), (3, 2)))
    tiles = gaussian(splits[1], (NXC, NYC, SLOTS, NODES, NODES), (NODES * SLOTS) ** -0.5, 0.1875, ((0, 4), (1, 4)))
    codes = draw_codes(jax.random.fold_in(splits[5], 71), 0)
    counts = place_ends(jax.random.randint(splits[3], (NXC, NYC), 1, SLOTS + 1), jax.random.fold_in(splits[3], 1), 1, SLOTS).astype(jnp.int32)
    demo_nodes = place_ends(ranked(splits[4], (N_LON, N_LAT, DEMO * N_DEST), CLON * CLAT * NODES, 2), jax.random.fold_in(splits[4], 3), 0, (CLON * CLAT * NODES) - 1).astype(jnp.int32)
    return {"start_visits": start_visits, "tiles": tiles, "codes": codes, "counts": counts, "demo_nodes": demo_nodes}


def propagate(state, tiles, codes, counts):
    wrapped = jnp.concatenate([state[-1:], state, state[:1]], axis=0)
    padded = jnp.pad(wrapped, ((0, 0), (1, 1), (0, 0), (0, 0)))
    width = padded.shape[1]
    slot_ids = jnp.arange(SLOTS, dtype=jnp.int32)

    def column(row):
        window = lax.dynamic_slice_in_dim(padded, row.astype(jnp.int32), 3, 0)
        flat = window.reshape((3 * width,) + window.shape[2:])
        row_codes = lax.dynamic_index_in_dim(codes, row, 0, keepdims=False)
        row_counts = lax.dynamic_index_in_dim(counts, row, 0, keepdims=False)
        row_tiles = lax.dynamic_index_in_dim(tiles, row, 0, keepdims=False)
        offset_x = row_codes // 3
        offset_y = row_codes % 3
        ycoord = jnp.arange(row_codes.shape[0], dtype=jnp.int32)[:, None]
        index = (offset_x * width + ycoord + offset_y).astype(jnp.int32)
        source = flat[index]
        used = slot_ids[None, :] < row_counts[:, None]
        source = jnp.where(used[:, :, None, None], source, jnp.zeros_like(source))
        result = jnp.einsum("bkid,bkij->bjd", source.astype(jnp.float32), row_tiles.astype(jnp.float32))
        return result.astype(jnp.bfloat16)

    return lax.map(column, jnp.arange(state.shape[0], dtype=jnp.int32))


def reference(start_visits, tiles, codes, counts, demo_nodes):
    state = start_visits
    expected = jnp.zeros(start_visits.shape[:3], jnp.float32)
    for step in range(STEPS):
        state = propagate(state, tiles, codes, counts)
        expected = expected + jnp.sum(state.astype(jnp.float32), axis=-1)
    region_nodes = jnp.arange(CLON * CLAT * NODES, dtype=jnp.int32)
    listed = demo_nodes.reshape((N_LON * N_LAT, demo_nodes.shape[-1]))

    def tally(ids):
        return jnp.sum((ids[:, None] == region_nodes[None, :]).astype(jnp.float32), axis=0)

    tallied = lax.map(tally, listed)
    tallied = tallied.reshape((N_LON, N_LAT, CLON, CLAT, NODES)).transpose((0, 2, 1, 3, 4))
    demo_count = tallied.reshape((N_LON * CLON, N_LAT * CLAT, NODES))
    scale = (DESTG * N_DEST) ** -0.5
    return state, scale * (demo_count - expected)
```

```python
import functools

import jax
import jax.numpy as jnp
from jax import lax
from jax.experimental import pallas as pl
from jax.experimental.pallas import tpu as pltpu
from jax.sharding import PartitionSpec as P

STEPS = 4
VMEM = pltpu.VMEM
LIMIT = 24 * 1024 * 1024


def pairs(peers):
    if peers % 2 == 0:
        first = [(i, i ^ 1) for i in range(peers)]
        second = [(i, (i + 1) % peers if i % 2 else (i - 1) % peers) for i in range(peers)]
        return first, second
    up = [(i, (i + 1) % peers) for i in range(peers)]
    return up, [(j, i) for i, j in up]


def sides(axis):
    peers, me = lax.axis_size(axis), lax.axis_index(axis)
    if peers % 2 == 0:
        return me % 2, me % 2
    return jnp.int32(0), jnp.int32(1)


def swap(messages, axis):
    return [lax.ppermute(m, axis, p) for m, p in zip(messages, pairs(lax.axis_size(axis)))]


def call(kernel, name, outs, smem, vmem, flops=0, extra=()):
    spec = lambda space: pl.BlockSpec(memory_space=space)
    vmem = [pltpu.with_memory_space_constraint(v, VMEM) for v in vmem]
    moved = sum(v.size * v.dtype.itemsize for v in vmem)
    return pl.pallas_call(
        kernel,
        name=name,
        out_shape=[VMEM(s, d) for s, d in outs],
        in_specs=[spec(pltpu.SMEM)] * len(smem) + [spec(VMEM)] * len(vmem),
        out_specs=[spec(VMEM)] * len(outs),
        scratch_shapes=list(extra),
        compiler_params=pltpu.CompilerParams(vmem_limit_bytes=LIMIT),
        cost_estimate=pl.CostEstimate(flops=flops, bytes_accessed=moved, transcendentals=0),
    )(*smem, *vmem)


def put_edges(sel, at, along, shape, state, refs):
    columns, rows = shape
    for m, ref in enumerate(refs):
        up = sel[at] == m
        if along == 0:
            x = jnp.where(up, columns - 1, 0)
            for y in range(rows):
                ref[y] = state[x * rows + y]
        else:
            y = jnp.where(up, rows - 1, 0)
            for x in range(columns):
                ref[x] = state[x * rows + y]


def prep_kernel(shape, half, sel, start, xa, xb, pa0, pa1, pb0, pb1):
    for c in range(shape[0] * shape[1]):
        turned = start[c].T
        xa[c] = turned[:half]
        xb[c] = turned[half:]
    put_edges(sel, 0, 0, shape, xa, (pa0, pa1))
    put_edges(sel, 1, 1, shape, xb, (pb0, pb1))


def wide_kernel(shape, along, sel, state, r0, r1, q0, q1):
    columns, rows = shape
    other = 1 - along
    low_first = sel[2 + along] == 1
    for m, ref in enumerate((q0, q1)):
        up = sel[other] == m
        count = columns if along == 0 else rows
        place = jnp.where(up, (rows if along == 0 else columns) - 1, 0)
        ref[0] = jnp.where(low_first, r0[place], r1[place])
        ref[count + 1] = jnp.where(low_first, r1[place], r0[place])
        for i in range(count):
            ref[i + 1] = state[i * rows + place if along == 0 else place * rows + i]


def step_kernel(shape, slots, along, last, *refs):
    columns, rows = shape
    clusters = columns * rows
    sel, idx, state, r0, r1, q0, q1, tiles, tot = refs[:9]
    if last == 2:
        demo, other, scale = refs[9], refs[10], None
        out, grad, pool = refs[11:]
    elif last == 1:
        new, tot_out, pool = refs[9:]
    else:
        new, s0, s1, tot_out, pool = refs[9:]
    at = 0
    for part in (state, r0, r1, q0, q1):
        for i in range(part.shape[0]):
            pool[at + i] = part[i]
        at += part.shape[0]
    pool[at] = jnp.zeros(pool.shape[1:], pool.dtype)
    half, nodes = pool.shape[1:]
    for c in range(clusters):
        lhs = jnp.concatenate([pool[idx[c * slots + k]] for k in range(slots)], axis=1)
        acc = jnp.dot(lhs, tiles[c], preferred_element_type=jnp.float32)
        value = acc.astype(jnp.bfloat16)
        sums = value.astype(jnp.float32).reshape(half // 8, 8, nodes).sum(axis=0)
        if last == 2:
            out[c] = jnp.concatenate([other[c], value], axis=0).T
            grad[pl.ds(c, 1), :] = demo[pl.ds(c, 1), :] - (tot[c] + sums).sum(axis=0, keepdims=True)
        else:
            new[c] = value
            tot_out[c] = tot[c] + sums
    if last == 0:
        put_edges(sel, along, along, shape, new, (s0, s1))


def demo_kernel(nodes_ref, counts_ref):
    listed = nodes_ref[...]
    high, low = counts_ref.shape
    entries = listed.shape[1]
    up = lax.broadcasted_iota(jnp.int32, (high, entries), 0) == listed // low
    down = lax.broadcasted_iota(jnp.int32, (low, entries), 0) == listed % low
    counts_ref[...] = lax.dot_general(
        up.astype(jnp.bfloat16),
        down.astype(jnp.bfloat16),
        (((1,), (1,)), ((), ())),
        preferred_element_type=jnp.float32,
    )


def on_device(start_visits, tiles, codes, counts, demo_nodes):
    columns, rows, nodes, dests = start_visits.shape
    slots = codes.shape[-1]
    clusters = columns * rows
    shape = (columns, rows)
    half = dests // 2
    scale = (lax.axis_size("dest") * dests) ** (-0.5)

    up_lon, hi_lon = sides("lon")
    up_lat, hi_lat = sides("lat")
    sel = jnp.stack([up_lon, up_lat, hi_lon, hi_lat]).astype(jnp.int32)

    xcoord = jnp.arange(columns, dtype=jnp.int32)[:, None, None]
    ycoord = jnp.arange(rows, dtype=jnp.int32)[None, :, None]
    sx, sy = xcoord + codes // 3 - 1, ycoord + codes % 3 - 1
    inx = jnp.logical_and(sx >= 0, sx < columns)
    iny = jnp.logical_and(sy >= 0, sy < rows)
    slot_lon = jnp.where(sx < 0, 1 - hi_lon, hi_lon)
    slot_lat = jnp.where(sy < 0, 1 - hi_lat, hi_lat)
    band, bands = lax.axis_index("lat"), lax.axis_size("lat")
    outside = jnp.logical_or(
        jnp.logical_and(band == 0, sy < 0), jnp.logical_and(band == bands - 1, sy >= rows)
    )
    unused = jnp.arange(slots, dtype=jnp.int32)[None, None, :] >= counts[:, :, None]
    drop = jnp.logical_or(outside, unused)
    own = sx * rows + sy
    first_a = clusters + slot_lon * rows + sy
    second_a = clusters + 2 * rows + slot_lat * (columns + 2) + sx + 1
    zero_a = clusters + 2 * rows + 2 * (columns + 2)
    idx_a = jnp.where(drop, zero_a, jnp.where(iny, jnp.where(inx, own, first_a), second_a))
    first_b = clusters + slot_lat * columns + sx
    second_b = clusters + 2 * columns + slot_lon * (rows + 2) + sy + 1
    zero_b = clusters + 2 * columns + 2 * (rows + 2)
    idx_b = jnp.where(drop, zero_b, jnp.where(inx, jnp.where(iny, own, first_b), second_b))
    idx = [idx_a.reshape(-1), idx_b.reshape(-1)]
    pool = [zero_a + 1, zero_b + 1]

    bf, f32 = jnp.bfloat16, jnp.float32
    block = lambda n: ((n, half, nodes), bf)
    low = min(nodes, 128)
    (demo,) = call(
        demo_kernel, "demo", [((clusters * nodes // low, low), f32)], [], [demo_nodes.reshape(1, -1)]
    )
    demo = demo.reshape(clusters, nodes)
    weights = tiles.reshape(clusters, slots * nodes, nodes)
    tot = jnp.zeros((clusters, 8, nodes), f32)
    xa, xb, pa0, pa1, pb0, pb1 = call(
        functools.partial(prep_kernel, shape, half),
        "prep",
        [block(clusters), block(clusters), block(rows), block(rows), block(columns), block(columns)],
        [sel],
        [start_visits.reshape(clusters, nodes, dests)],
    )
    state, message = [xa, xb], [(pa0, pa1), (pb0, pb1)]
    axes = ("lon", "lat")
    flops = 2 * clusters * slots * nodes * nodes * half
    for step in range(STEPS):
        first = [swap(message[s], axes[s]) for s in (0, 1)]
        wide = []
        for s in (0, 1):
            count = (columns if s == 0 else rows) + 2
            wide.append(
                call(
                    functools.partial(wide_kernel, shape, s),
                    f"wide{s}",
                    [block(count), block(count)],
                    [sel],
                    [state[s], *first[s]],
                )
            )
        second = [swap(wide[s], axes[1 - s]) for s in (0, 1)]
        for s in (0, 1):
            last = (s + 1) if step == STEPS - 1 else 0
            edge = rows if s == 0 else columns
            outs = [block(clusters), block(edge), block(edge), ((clusters, 8, nodes), f32)]
            extra = []
            if last == 1:
                outs = [outs[0], outs[3]]
            elif last == 2:
                outs = [((clusters, nodes, dests), bf), ((clusters, nodes), f32)]
                extra = [demo, state[0]]
            got = call(
                functools.partial(step_kernel, shape, slots, s, last),
                f"step{s}",
                outs,
                [sel, idx[s]],
                [state[s], *first[s], *second[s], weights, tot, *extra],
                flops=flops,
                extra=[VMEM((pool[s], half, nodes), bf)],
            )
            if last == 2:
                visits, grad = got
            elif last == 1:
                state[s], tot = got
            else:
                state[s], tot = got[0], got[3]
                message[s] = (got[1], got[2])
    grad = scale * grad
    peers = lax.axis_size("dest")
    if peers == 2:
        grad = grad + lax.ppermute(grad, "dest", [(0, 1), (1, 0)])
    else:
        grad = lax.psum(grad, "dest")
    return visits.reshape(start_visits.shape), grad.reshape(columns, rows, nodes)


def solution(mesh):
    return jax.shard_map(
        on_device,
        mesh=mesh,
        in_specs=(
            P("lon", "lat", None, "dest"),
            P("lon", "lat", None, None, None),
            P("lon", "lat", None),
            P("lon", "lat"),
            P("lon", "lat", "dest"),
        ),
        out_specs=(P("lon", "lat", None, "dest"), P("lon", "lat", None)),
        check_vma=False,
    )
```

```python
import functools

import jax
import jax.numpy as jnp
from jax import lax
from jax.experimental import pallas as pl
from jax.experimental.pallas import tpu as pltpu
from jax.sharding import PartitionSpec as P

STEPS = 4
VMEM = pltpu.VMEM
AXES = ("lon", "lat")
LIMIT = 24 * 1024 * 1024


def pairs(peers):
    if peers % 2 == 0:
        first = [(i, i ^ 1) for i in range(peers)]
        second = [(i, (i + 1) % peers if i % 2 else (i - 1) % peers) for i in range(peers)]
        return first, second
    up = [(i, (i + 1) % peers) for i in range(peers)]
    return up, [(j, i) for i, j in up]


def sides(axis):
    peers, me = lax.axis_size(axis), lax.axis_index(axis)
    if peers % 2 == 0:
        return me % 2, me % 2
    return jnp.int32(0), jnp.int32(1)


def swap(messages, axis):
    return [lax.ppermute(m, axis, p) for m, p in zip(messages, pairs(lax.axis_size(axis)))]


def call(kernel, name, outs, vmem, flops=0, extra=(), plain=0):
    spec = pl.BlockSpec(memory_space=VMEM)
    vmem = [pltpu.with_memory_space_constraint(v, VMEM) for v in vmem]
    moved = sum(v.size * v.dtype.itemsize for v in vmem)
    return pl.pallas_call(
        kernel,
        name=name,
        out_shape=[jax.ShapeDtypeStruct(*o) if i < plain else VMEM(*o) for i, o in enumerate(outs)],
        in_specs=[spec] * len(vmem),
        out_specs=[pl.BlockSpec(memory_space=pl.ANY)] * plain + [spec] * (len(outs) - plain),
        scratch_shapes=list(extra),
        compiler_params=pltpu.CompilerParams(vmem_limit_bytes=LIMIT),
        cost_estimate=pl.CostEstimate(flops=flops, bytes_accessed=moved, transcendentals=0),
    )(*vmem)


def hold_kernel(source, held, sem):
    copy = pltpu.make_async_copy(source, held, sem)
    copy.start()
    copy.wait()


def hold(array):
    return pl.pallas_call(
        hold_kernel,
        name="hold",
        out_shape=VMEM(array.shape, array.dtype),
        in_specs=[pl.BlockSpec(memory_space=pl.ANY)],
        out_specs=pl.BlockSpec(memory_space=VMEM),
        scratch_shapes=[pltpu.SemaphoreType.DMA],
        compiler_params=pltpu.CompilerParams(vmem_limit_bytes=LIMIT),
        cost_estimate=pl.CostEstimate(flops=1 << 22, bytes_accessed=array.size * 2, transcendentals=0),
    )(pltpu.with_memory_space_constraint(array, pltpu.HBM))


def put_edges(along, shape, state, refs):
    columns, rows = shape
    upward, _ = sides(AXES[along])
    for m, ref in enumerate(refs):
        up = upward == m
        if along == 0:
            x = jnp.where(up, columns - 1, 0)
            for y in range(rows):
                ref[y] = state[x * rows + y]
        else:
            y = jnp.where(up, rows - 1, 0)
            for x in range(columns):
                ref[x] = state[x * rows + y]


def prep_kernel(shape, half, start, xa, xb, pa0, pa1, pb0, pb1):
    for c in range(shape[0] * shape[1]):
        turned = start[c].T
        xa[c] = turned[:half]
        xb[c] = turned[half:]
    put_edges(0, shape, xa, (pa0, pa1))
    put_edges(1, shape, xb, (pb0, pb1))


def wide_kernel(shape, along, state, r0, r1, q0, q1):
    columns, rows = shape
    low_first = sides(AXES[along])[1] == 1
    upward, _ = sides(AXES[1 - along])
    for m, ref in enumerate((q0, q1)):
        up = upward == m
        count = columns if along == 0 else rows
        place = jnp.where(up, (rows if along == 0 else columns) - 1, 0)
        ref[0] = jnp.where(low_first, r0[place], r1[place])
        ref[count + 1] = jnp.where(low_first, r1[place], r0[place])
        for i in range(count):
            ref[i + 1] = state[i * rows + place if along == 0 else place * rows + i]


def step_kernel(shape, slots, along, last, *refs):
    columns, rows = shape
    clusters = columns * rows
    idx, state, r0, r1, q0, q1, tiles, tot = refs[:8]
    if last == 2:
        demo, other, out, grad, pool, turned, sems = refs[8:]
    elif last == 1:
        new, tot_out, pool = refs[8:]
    else:
        new, s0, s1, tot_out, pool = refs[8:]
    at = 0
    for part in (state, r0, r1, q0, q1):
        for i in range(part.shape[0]):
            pool[at + i] = part[i]
        at += part.shape[0]
    pool[at] = jnp.zeros(pool.shape[1:], pool.dtype)
    half, nodes = pool.shape[1:]
    for c in range(clusters):
        entries = [divmod(c * slots + k, 128) for k in range(slots)]
        picks = [idx[i : i + 1, :][0, j] for i, j in entries]
        lhs = jnp.concatenate([pool[p] for p in picks], axis=1)
        acc = jnp.dot(lhs, tiles[c], preferred_element_type=jnp.float32)
        value = acc.astype(jnp.bfloat16)
        sums = value.astype(jnp.float32).reshape(half // 8, 8, nodes).sum(axis=0)
        if last == 2:
            turned[c] = jnp.concatenate([other[c], value], axis=0).T
            pltpu.make_async_copy(turned.at[c], out.at[c], sems.at[c]).start()
            x, y = divmod(c, rows)
            parts = nodes // demo.shape[1]
            seen = jnp.concatenate([demo[i : i + 1, :] for i in range(c * parts, (c + 1) * parts)], axis=1)
            grad[x, y : y + 1, :] = seen - (tot[c] + sums).sum(axis=0, keepdims=True)
        else:
            new[c] = value
            tot_out[c] = tot[c] + sums
    if last == 2:
        for c in range(clusters):
            pltpu.make_async_copy(turned.at[c], out.at[c], sems.at[c]).wait()
    if last == 0:
        put_edges(along, shape, new, (s0, s1))


def demo_kernel(nodes_ref, counts_ref):
    listed = nodes_ref[...]
    high, low = counts_ref.shape
    entries = listed.shape[1]
    up = lax.broadcasted_iota(jnp.int32, (high, entries), 0) == listed // low
    down = lax.broadcasted_iota(jnp.int32, (low, entries), 0) == listed % low
    counts_ref[...] = lax.dot_general(
        up.astype(jnp.bfloat16),
        down.astype(jnp.bfloat16),
        (((1,), (1,)), ((), ())),
        preferred_element_type=jnp.float32,
    )


def on_device(start_visits, tiles, codes, counts, demo_nodes):
    columns, rows, nodes, dests = start_visits.shape
    slots = codes.shape[-1]
    clusters = columns * rows
    shape = (columns, rows)
    half = dests // 2
    scale = (lax.axis_size("dest") * dests) ** (-0.5)

    _, hi_lon = sides("lon")
    _, hi_lat = sides("lat")

    xcoord = jnp.arange(columns, dtype=jnp.int32)[:, None, None]
    ycoord = jnp.arange(rows, dtype=jnp.int32)[None, :, None]
    sx, sy = xcoord + codes // 3 - 1, ycoord + codes % 3 - 1
    inx = jnp.logical_and(sx >= 0, sx < columns)
    iny = jnp.logical_and(sy >= 0, sy < rows)
    slot_lon = jnp.where(sx < 0, 1 - hi_lon, hi_lon)
    slot_lat = jnp.where(sy < 0, 1 - hi_lat, hi_lat)
    band, bands = lax.axis_index("lat"), lax.axis_size("lat")
    outside = jnp.logical_or(
        jnp.logical_and(band == 0, sy < 0), jnp.logical_and(band == bands - 1, sy >= rows)
    )
    unused = jnp.arange(slots, dtype=jnp.int32)[None, None, :] >= counts[:, :, None]
    drop = jnp.logical_or(outside, unused)
    own = sx * rows + sy
    first_a = clusters + slot_lon * rows + sy
    second_a = clusters + 2 * rows + slot_lat * (columns + 2) + sx + 1
    zero_a = clusters + 2 * rows + 2 * (columns + 2)
    idx_a = jnp.where(drop, zero_a, jnp.where(iny, jnp.where(inx, own, first_a), second_a))
    first_b = clusters + slot_lat * columns + sx
    second_b = clusters + 2 * columns + slot_lon * (rows + 2) + sy + 1
    zero_b = clusters + 2 * columns + 2 * (rows + 2)
    idx_b = jnp.where(drop, zero_b, jnp.where(inx, jnp.where(iny, own, first_b), second_b))
    spare = -(clusters * slots) % 128
    idx = [jnp.pad(i.reshape(-1), (0, spare)).reshape(-1, 128) for i in (idx_a, idx_b)]
    pool = [zero_a + 1, zero_b + 1]

    bf, f32 = jnp.bfloat16, jnp.float32
    block = lambda n: ((n, half, nodes), bf)
    low = min(nodes, 128)
    (demo,) = call(
        demo_kernel, "demo", [((clusters * nodes // low, low), f32)], [demo_nodes.reshape(1, -1)]
    )
    weights = hold(tiles.reshape(clusters, slots * nodes, nodes))
    tot = jnp.zeros((clusters, 8, nodes), f32)
    xa, xb, pa0, pa1, pb0, pb1 = call(
        functools.partial(prep_kernel, shape, half),
        "prep",
        [block(clusters), block(clusters), block(rows), block(rows), block(columns), block(columns)],
        [start_visits.reshape(clusters, nodes, dests)],
    )
    state, message = [xa, xb], [(pa0, pa1), (pb0, pb1)]
    flops = 2 * clusters * slots * nodes * nodes * half
    for step in range(STEPS):
        first = [swap(message[s], AXES[s]) for s in (0, 1)]
        wide = []
        for s in (0, 1):
            count = (columns if s == 0 else rows) + 2
            wide.append(
                call(
                    functools.partial(wide_kernel, shape, s),
                    f"wide{s}",
                    [block(count), block(count)],
                    [state[s], *first[s]],
                )
            )
        second = [swap(wide[s], AXES[1 - s]) for s in (0, 1)]
        for s in (0, 1):
            last = (s + 1) if step == STEPS - 1 else 0
            edge = rows if s == 0 else columns
            outs = [block(clusters), block(edge), block(edge), ((clusters, 8, nodes), f32)]
            extra, plain, scratch = [], 0, [VMEM((pool[s], half, nodes), bf)]
            if last == 1:
                outs = [outs[0], outs[3]]
            elif last == 2:
                outs = [((clusters, nodes, dests), bf), ((columns, rows, nodes), f32)]
                extra, plain = [demo, state[0]], 1
                scratch += [VMEM((clusters, nodes, dests), bf), pltpu.SemaphoreType.DMA((clusters,))]
            got = call(
                functools.partial(step_kernel, shape, slots, s, last),
                f"step{s}",
                outs,
                [idx[s], state[s], *first[s], *second[s], weights, tot, *extra],
                flops=flops,
                extra=scratch,
                plain=plain,
            )
            if last == 2:
                visits, grad = got
            elif last == 1:
                state[s], tot = got
            else:
                state[s], tot = got[0], got[3]
                message[s] = (got[1], got[2])
    grad = scale * grad
    peers = lax.axis_size("dest")
    if peers == 2:
        grad = grad + lax.ppermute(grad, "dest", [(0, 1), (1, 0)])
    else:
        grad = lax.psum(grad, "dest")
    return visits.reshape(start_visits.shape), grad


def solution(mesh):
    return jax.shard_map(
        on_device,
        mesh=mesh,
        in_specs=(
            P("lon", "lat", None, "dest"),
            P("lon", "lat", None, None, None),
            P("lon", "lat", None),
            P("lon", "lat"),
            P("lon", "lat", "dest"),
        ),
        out_specs=(P("lon", "lat", None, "dest"), P("lon", "lat", None)),
        check_vma=False,
    )
```

```python
import functools

import jax
import jax.numpy as jnp
from jax import lax
from jax.experimental import pallas as pl
from jax.experimental.pallas import tpu as pltpu
from jax.sharding import PartitionSpec as P


STEPS = 4
VMEM = pltpu.VMEM
ANY = pl.ANY
LIMIT = 24 * 1024 * 1024


def pairs(peers):
    if peers % 2 == 0:
        first = [(i, i ^ 1) for i in range(peers)]
        second = [(i, (i + 1) % peers if i % 2 else (i - 1) % peers) for i in range(peers)]
        return first, second
    up = [(i, (i + 1) % peers) for i in range(peers)]
    return up, [(j, i) for i, j in up]


def sides(axis):
    peers, me = lax.axis_size(axis), lax.axis_index(axis)
    if peers % 2 == 0:
        return me % 2, me % 2
    return jnp.int32(0), jnp.int32(1)


def swap(messages, axis):
    received = []
    for message, moves in zip(messages, pairs(lax.axis_size(axis))):
        received.append(lax.ppermute(message, axis, moves))
    return received


def call(kernel, outs, args, flops=0, scratch=(), same=None, plain=()):
    same = same or {}
    loose = {i for i, o in same.items() if o in plain}
    args = [a if i in loose else pltpu.with_memory_space_constraint(a, VMEM) for i, a in enumerate(args)]
    spec = lambda free: pl.BlockSpec(memory_space=ANY if free else VMEM)
    return pl.pallas_call(
        kernel,
        out_shape=[jax.ShapeDtypeStruct(*o) if i in plain else VMEM(*o) for i, o in enumerate(outs)],
        in_specs=[spec(i in loose) for i in range(len(args))],
        out_specs=[spec(i in plain) for i in range(len(outs))],
        scratch_shapes=list(scratch),
        input_output_aliases=same,
        compiler_params=pltpu.CompilerParams(vmem_limit_bytes=LIMIT),
        cost_estimate=pl.CostEstimate(flops=flops, bytes_accessed=1 << 20, transcendentals=0),
    )(*args)


def hold_kernel(source, held, sem):
    copy = pltpu.make_async_copy(source, held, sem)
    copy.start()
    copy.wait()


def hold(array):
    return pl.pallas_call(
        hold_kernel,
        name="hold",
        out_shape=VMEM(array.shape, array.dtype),
        in_specs=[pl.BlockSpec(memory_space=ANY)],
        out_specs=pl.BlockSpec(memory_space=VMEM),
        scratch_shapes=[pltpu.SemaphoreType.DMA],
        compiler_params=pltpu.CompilerParams(vmem_limit_bytes=LIMIT),
        cost_estimate=pl.CostEstimate(flops=1 << 22, bytes_accessed=array.size * 2, transcendentals=0),
    )(pltpu.with_memory_space_constraint(array, pltpu.HBM))


def put_edges(shape, state, messages):
    columns, rows = shape
    lon, lat = sides("lon")[0], sides("lat")[0]
    for m in (0, 1):
        x = jnp.where(lon == m, columns - 1, 0)
        for y in range(rows):
            messages[m][y] = state[x * rows + y]
        y = jnp.where(lat == m, rows - 1, 0)
        for x in range(columns):
            messages[2 + m][x] = state[x * rows + y]


def prep_kernel(shape, start, state, *messages):
    for c in range(shape[0] * shape[1]):
        state[c] = start[c].T
    put_edges(shape, state, messages)


def corner_kernel(rows, r0, r1, q0, q1):
    low_first = sides("lon")[1] == 1
    upward = sides("lat")[0]
    for m, ref in enumerate((q0, q1)):
        y = jnp.where(upward == m, rows - 1, 0)
        ref[0] = jnp.where(low_first, r0[y], r1[y])
        ref[1] = jnp.where(low_first, r1[y], r0[y])


def corner_places(shape):
    columns, rows = shape
    ends = {x * rows + y for x in (0, columns - 1) for y in (0, rows - 1)}
    return sorted(ends)


def cluster(c, slots, idx, pool, tiles):
    entries = [divmod(c * slots + k, 128) for k in range(slots)]
    picks = [idx[i : i + 1, :][0, j] for i, j in entries]
    lhs = jnp.concatenate([pool[p] for p in picks], axis=1)
    value = jnp.dot(lhs, tiles[c], preferred_element_type=jnp.float32).astype(jnp.bfloat16)
    share, nodes = value.shape
    return value, value.astype(jnp.float32).reshape(share // 8, 8, nodes).sum(axis=0)


def emit(places, shape, slots, idx, pool, tiles, tot, results, last):
    if last:
        demo, out, grad, turned, sems = results
        for c in places:
            value, sums = cluster(c, slots, idx, pool, tiles)
            turned[c] = value.T
            pltpu.make_async_copy(turned.at[c], out.at[c], sems.at[c]).start()
            x, y = divmod(c, shape[1])
            parts = value.shape[1] // demo.shape[1]
            seen = jnp.concatenate([demo[i : i + 1, :] for i in range(c * parts, (c + 1) * parts)], axis=1)
            grad[x, y : y + 1, :] = seen - (tot[c] + sums).sum(axis=0, keepdims=True)
        for c in places:
            pltpu.make_async_copy(turned.at[c], out.at[c], sems.at[c]).wait()
    else:
        new, tot_out = results
        for c in places:
            value, sums = cluster(c, slots, idx, pool, tiles)
            new[c] = value
            tot_out[c] = tot[c] + sums


def main_kernel(shape, slots, last, *refs):
    idx, state, *halo, tiles, tot = refs[:8]
    clusters = shape[0] * shape[1]
    if last:
        demo, out, grad, pool, turned, sems = refs[8:]
        results = demo, out, grad, turned, sems
    else:
        new, tot_out, pool = refs[8:]
        results = new, tot_out
    at = 0
    for part in (state, *halo):
        for i in range(part.shape[0]):
            pool[at + i] = part[i]
        at += part.shape[0]
    pool[at] = jnp.zeros(pool.shape[1:], pool.dtype)
    corners = corner_places(shape)
    emit([c for c in range(clusters) if c not in corners], shape, slots, idx, pool, tiles, tot, results, last)


def tail_kernel(shape, slots, last, *refs):
    idx, q0, q1, tiles, tot, _, _, _ = refs[:8]
    if last:
        demo, out, grad, pool, turned, sems = refs[8:]
        results = demo, out, grad, turned, sems
    else:
        new, tot_out, pool, *messages = refs[8:]
        results = new, tot_out
    at = pool.shape[0] - 4
    for i, (part, j) in enumerate(((q0, 0), (q0, 1), (q1, 0), (q1, 1))):
        pool[at + i] = part[j]
    emit(corner_places(shape), shape, slots, idx, pool, tiles, tot, results, last)
    if not last:
        put_edges(shape, new, messages)


def demo_kernel(nodes_ref, counts_ref):
    listed = nodes_ref[...]
    high, low = counts_ref.shape
    entries = listed.shape[1]
    up = lax.broadcasted_iota(jnp.int32, (high, entries), 0) == listed // low
    down = lax.broadcasted_iota(jnp.int32, (low, entries), 0) == listed % low
    counts_ref[...] = lax.dot_general(
        up.astype(jnp.bfloat16),
        down.astype(jnp.bfloat16),
        (((1,), (1,)), ((), ())),
        preferred_element_type=jnp.float32,
    )


def sources(codes, counts, shape):
    columns, rows = shape
    clusters = columns * rows
    slots = codes.shape[-1]
    hi_lon, hi_lat = sides("lon")[1], sides("lat")[1]
    xcoord = jnp.arange(columns, dtype=jnp.int32)[:, None, None]
    ycoord = jnp.arange(rows, dtype=jnp.int32)[None, :, None]
    sx, sy = xcoord + codes // 3 - 1, ycoord + codes % 3 - 1
    inx = jnp.logical_and(sx >= 0, sx < columns)
    iny = jnp.logical_and(sy >= 0, sy < rows)
    by_lon = jnp.where(sx < 0, 1 - hi_lon, hi_lon)
    by_lat = jnp.where(sy < 0, 1 - hi_lat, hi_lat)
    band, bands = lax.axis_index("lat"), lax.axis_size("lat")
    outside = jnp.logical_or(
        jnp.logical_and(band == 0, sy < 0), jnp.logical_and(band == bands - 1, sy >= rows)
    )
    unused = jnp.arange(slots, dtype=jnp.int32)[None, None, :] >= counts[:, :, None]
    second = clusters + 2 * rows
    zero = second + 2 * columns
    source = jnp.where(
        iny,
        jnp.where(inx, sx * rows + sy, clusters + by_lon * rows + sy),
        jnp.where(inx, second + by_lat * columns + sx, zero + 1 + by_lat * 2 + (sx >= columns)),
    )
    source = jnp.where(jnp.logical_or(outside, unused), zero, source).reshape(-1)
    return jnp.pad(source, (0, -source.size % 128)).reshape(-1, 128), zero + 5


def on_device(start_visits, tiles, codes, counts, demo_nodes):
    columns, rows, nodes, dests = start_visits.shape
    slots = codes.shape[-1]
    clusters = columns * rows
    shape = (columns, rows)
    scale = (lax.axis_size("dest") * dests) ** (-0.5)
    idx, depth = sources(codes, counts, shape)

    bf, f32 = jnp.bfloat16, jnp.float32
    block = lambda n: ((n, dests, nodes), bf)
    low = min(nodes, 128)
    (demo,) = call(demo_kernel, [((clusters * nodes // low, low), f32)], [demo_nodes.reshape(1, -1)])
    weights = hold(tiles.reshape(clusters, slots * nodes, nodes))
    tot = jnp.zeros((clusters, 8, nodes), f32)
    sums = (tot.shape, f32)
    edges = [block(rows)] * 2 + [block(columns)] * 2
    state, *messages = call(
        functools.partial(prep_kernel, shape), [block(clusters), *edges], [start_visits.reshape(clusters, nodes, dests)]
    )
    work = 2 * clusters * slots * nodes * nodes * dests
    for step in range(STEPS):
        last = step == STEPS - 1
        lon = swap(messages[:2], "lon")
        lat = swap(messages[2:], "lat")
        ends = call(functools.partial(corner_kernel, rows), [block(2)] * 2, lon)
        ends = swap(ends, "lat")
        main = functools.partial(main_kernel, shape, slots, last)
        tail = functools.partial(tail_kernel, shape, slots, last)
        given = [idx, state, *lon, *lat, weights, tot]
        if last:
            outs = [((clusters, nodes, dests), bf), ((columns, rows, nodes), f32), block(depth)]
            scratch = [VMEM((clusters, nodes, dests), bf), pltpu.SemaphoreType.DMA((clusters,))]
            visits, grad, pool = call(main, outs, [*given, demo], work * 3 // 4, scratch, plain=(0,))
            visits, grad, _ = call(
                tail,
                outs,
                [idx, *ends, weights, tot, visits, grad, pool, demo],
                work // 4,
                scratch,
                same={5: 0, 6: 1, 7: 2},
                plain=(0,),
            )
        else:
            outs = [block(clusters), sums, block(depth)]
            new, tot_new, pool = call(main, outs, given, work * 3 // 4)
            state, tot, _, *messages = call(
                tail, outs + edges, [idx, *ends, weights, tot, new, tot_new, pool], work // 4, same={5: 0, 6: 1, 7: 2}
            )
    grad = scale * grad
    if lax.axis_size("dest") == 2:
        grad = grad + lax.ppermute(grad, "dest", [(0, 1), (1, 0)])
    else:
        grad = lax.psum(grad, "dest")
    return visits.reshape(start_visits.shape), grad


def solution(mesh):
    return jax.shard_map(
        on_device,
        mesh=mesh,
        in_specs=(
            P("lon", "lat", None, "dest"),
            P("lon", "lat", None, None, None),
            P("lon", "lat", None),
            P("lon", "lat"),
            P("lon", "lat", "dest"),
        ),
        out_specs=(P("lon", "lat", None, "dest"), P("lon", "lat", None)),
        check_vma=False,
    )
```

```python
import functools

import jax
import jax.numpy as jnp
from jax import lax
from jax.experimental import pallas as pl
from jax.experimental.pallas import tpu as pltpu
from jax.sharding import PartitionSpec as P


STEPS = 4
VMEM = pltpu.VMEM
ANY = pl.ANY
LIMIT = 24 * 1024 * 1024


def pairs(peers):
    if peers % 2 == 0:
        first = [(i, i ^ 1) for i in range(peers)]
        second = [(i, (i + 1) % peers if i % 2 else (i - 1) % peers) for i in range(peers)]
        return first, second
    up = [(i, (i + 1) % peers) for i in range(peers)]
    return up, [(j, i) for i, j in up]


def sides(axis):
    peers, me = lax.axis_size(axis), lax.axis_index(axis)
    if peers % 2 == 0:
        return me % 2, me % 2
    return jnp.int32(0), jnp.int32(1)


def swap(messages, axis):
    received = []
    for message, moves in zip(messages, pairs(lax.axis_size(axis))):
        received.append(lax.ppermute(message, axis, moves))
    return received


def call(kernel, outs, args, flops=0, scratch=(), same=None, plain=()):
    same = same or {}
    loose = {i for i, o in same.items() if o in plain}
    args = [a if i in loose else pltpu.with_memory_space_constraint(a, VMEM) for i, a in enumerate(args)]
    spec = lambda free: pl.BlockSpec(memory_space=ANY if free else VMEM)
    return pl.pallas_call(
        kernel,
        out_shape=[jax.ShapeDtypeStruct(*o) if i in plain else VMEM(*o) for i, o in enumerate(outs)],
        in_specs=[spec(i in loose) for i in range(len(args))],
        out_specs=[spec(i in plain) for i in range(len(outs))],
        scratch_shapes=list(scratch),
        input_output_aliases=same,
        compiler_params=pltpu.CompilerParams(vmem_limit_bytes=LIMIT),
        cost_estimate=pl.CostEstimate(flops=flops, bytes_accessed=1 << 20, transcendentals=0),
    )(*args)


def hold_kernel(source, held, sem):
    copy = pltpu.make_async_copy(source, held, sem)
    copy.start()
    copy.wait()


def hold(array):
    return pl.pallas_call(
        hold_kernel,
        name="hold",
        out_shape=VMEM(array.shape, array.dtype),
        in_specs=[pl.BlockSpec(memory_space=ANY)],
        out_specs=pl.BlockSpec(memory_space=VMEM),
        scratch_shapes=[pltpu.SemaphoreType.DMA],
        compiler_params=pltpu.CompilerParams(vmem_limit_bytes=LIMIT),
        cost_estimate=pl.CostEstimate(flops=1 << 22, bytes_accessed=array.size * 2, transcendentals=0),
    )(pltpu.with_memory_space_constraint(array, pltpu.HBM))


def put_lon(shape, state, messages, places):
    columns, rows = shape
    for m, ref in enumerate(messages):
        x = jnp.where(sides("lon")[0] == m, columns - 1, 0)
        for i, y in enumerate(places):
            ref[i] = state[x * rows + y]


def put_edges(shape, state, messages):
    columns, rows = shape
    put_lon(shape, state, messages[:2], (0, rows - 1))
    for m, ref in enumerate(messages[2:]):
        y = jnp.where(sides("lat")[0] == m, rows - 1, 0)
        for x in range(columns):
            ref[x] = state[x * rows + y]


def prep_kernel(shape, start, state, *messages):
    for c in range(shape[0] * shape[1]):
        state[c] = start[c].T
    put_lon(shape, state, messages[:2], range(1, shape[1] - 1))
    put_edges(shape, state, messages[2:])


def corner_kernel(r0, r1, q0, q1):
    low_first = sides("lon")[1] == 1
    upward = sides("lat")[0]
    for m, ref in enumerate((q0, q1)):
        end = jnp.where(upward == m, 1, 0)
        ref[0] = jnp.where(low_first, r0[end], r1[end])
        ref[1] = jnp.where(low_first, r1[end], r0[end])


def corner_places(shape):
    columns, rows = shape
    ends = {x * rows + y for x in (0, columns - 1) for y in (0, rows - 1)}
    return sorted(ends)


def cluster(c, slots, idx, pool, tiles):
    entries = [divmod(c * slots + k, 128) for k in range(slots)]
    picks = [idx[i : i + 1, :][0, j] for i, j in entries]
    lhs = jnp.concatenate([pool[p] for p in picks], axis=1)
    value = jnp.dot(lhs, tiles[c], preferred_element_type=jnp.float32).astype(jnp.bfloat16)
    share, nodes = value.shape
    return value, value.astype(jnp.float32).reshape(share // 8, 8, nodes).sum(axis=0)


def emit(places, shape, slots, idx, pool, tiles, tot, results, last):
    if last:
        demo, out, grad, turned, sems, scale = results
        copies = []
        for i, c in enumerate(places):
            value, sums = cluster(c, slots, idx, pool, tiles)
            turned[i] = value.T
            if out is not None:
                copies.append(pltpu.make_async_copy(turned.at[i], out.at[c], sems.at[i]))
                copies[-1].start()
            x, y = divmod(c, shape[1])
            parts = value.shape[1] // demo.shape[1]
            seen = jnp.concatenate([demo[i : i + 1, :] for i in range(c * parts, (c + 1) * parts)], axis=1)
            grad[x, y : y + 1, :] = scale * (seen - (tot[c] + sums).sum(axis=0, keepdims=True))
        for copy in copies:
            copy.wait()
    else:
        new, tot_out = results
        for c in places:
            value, sums = cluster(c, slots, idx, pool, tiles)
            new[c] = value
            tot_out[c] = tot[c] + sums


def main_kernel(shape, slots, last, scale, *refs):
    idx, state, *halo, tiles, tot = refs[:10]
    clusters = shape[0] * shape[1]
    if last:
        demo, out, grad, pool, turned, sems = refs[10:]
        results = demo, out, grad, turned, sems, scale
    else:
        new, tot_out, pool, *middle = refs[10:]
        results = new, tot_out
    at = 0
    for part in (state, *halo):
        for i in range(part.shape[0]):
            pool[at + i] = part[i]
        at += part.shape[0]
    pool[at] = jnp.zeros(pool.shape[1:], pool.dtype)
    corners = corner_places(shape)
    emit([c for c in range(clusters) if c not in corners], shape, slots, idx, pool, tiles, tot, results, last)
    if not last:
        put_lon(shape, new, middle, range(1, shape[1] - 1))


def tail_kernel(shape, slots, last, scale, *refs):
    idx, q0, q1, tiles, tot = refs[:5]
    if last:
        _, _, demo, grad, pool, turned = refs[5:]
        results = demo, None, grad, turned, None, scale
    else:
        _, _, _, new, tot_out, pool, *messages = refs[5:]
        results = new, tot_out
    at = pool.shape[0] - 4
    for i, (part, j) in enumerate(((q0, 0), (q0, 1), (q1, 0), (q1, 1))):
        pool[at + i] = part[j]
    emit(corner_places(shape), shape, slots, idx, pool, tiles, tot, results, last)
    if not last:
        put_edges(shape, new, messages)


def flush_kernel(places, turned, _, out, sems):
    copies = [pltpu.make_async_copy(turned.at[i], out.at[c], sems.at[i]) for i, c in enumerate(places)]
    for copy in copies:
        copy.start()
    for copy in copies:
        copy.wait()


def demo_kernel(nodes_ref, counts_ref):
    listed = nodes_ref[...]
    high, low = counts_ref.shape
    entries = listed.shape[1]
    up = lax.broadcasted_iota(jnp.int32, (high, entries), 0) == listed // low
    down = lax.broadcasted_iota(jnp.int32, (low, entries), 0) == listed % low
    counts_ref[...] = lax.dot_general(
        up.astype(jnp.bfloat16),
        down.astype(jnp.bfloat16),
        (((1,), (1,)), ((), ())),
        preferred_element_type=jnp.float32,
    )


def sources(codes, counts, shape):
    columns, rows = shape
    clusters = columns * rows
    slots = codes.shape[-1]
    hi_lon, hi_lat = sides("lon")[1], sides("lat")[1]
    xcoord = jnp.arange(columns, dtype=jnp.int32)[:, None, None]
    ycoord = jnp.arange(rows, dtype=jnp.int32)[None, :, None]
    sx, sy = xcoord + codes // 3 - 1, ycoord + codes % 3 - 1
    inx = jnp.logical_and(sx >= 0, sx < columns)
    iny = jnp.logical_and(sy >= 0, sy < rows)
    by_lon = jnp.where(sx < 0, 1 - hi_lon, hi_lon)
    by_lat = jnp.where(sy < 0, 1 - hi_lat, hi_lat)
    band, bands = lax.axis_index("lat"), lax.axis_size("lat")
    outside = jnp.logical_or(
        jnp.logical_and(band == 0, sy < 0), jnp.logical_and(band == bands - 1, sy >= rows)
    )
    unused = jnp.arange(slots, dtype=jnp.int32)[None, None, :] >= counts[:, :, None]
    second = clusters + 2 * rows
    at_end = jnp.logical_or(sy == 0, sy == rows - 1)
    ends = clusters + by_lon * 2 + (sy > 0)
    between = clusters + 4 + by_lon * (rows - 2) + sy - 1
    zero = second + 2 * columns
    source = jnp.where(
        iny,
        jnp.where(inx, sx * rows + sy, jnp.where(at_end, ends, between)),
        jnp.where(inx, second + by_lat * columns + sx, zero + 1 + by_lat * 2 + (sx >= columns)),
    )
    source = jnp.where(jnp.logical_or(outside, unused), zero, source).reshape(-1)
    return jnp.pad(source, (0, -source.size % 128)).reshape(-1, 128), zero + 5


def on_device(start_visits, tiles, codes, counts, demo_nodes):
    columns, rows, nodes, dests = start_visits.shape
    slots = codes.shape[-1]
    clusters = columns * rows
    shape = (columns, rows)
    scale = (lax.axis_size("dest") * dests) ** (-0.5)
    idx, depth = sources(codes, counts, shape)

    bf, f32 = jnp.bfloat16, jnp.float32
    block = lambda n: ((n, dests, nodes), bf)
    low = min(nodes, 128)
    (demo,) = call(demo_kernel, [((clusters * nodes // low, low), f32)], [demo_nodes.reshape(1, -1)])
    tot = jnp.zeros((clusters, 8, nodes), f32)
    sums = (tot.shape, f32)
    middle = [block(rows - 2)] * 2
    edges = [block(2)] * 2 + [block(columns)] * 2
    state, mid0, mid1, *messages = call(
        functools.partial(prep_kernel, shape),
        [block(clusters), *middle, *edges],
        [start_visits.reshape(clusters, nodes, dests)],
    )
    work = 2 * clusters * slots * nodes * nodes * dests
    for step in range(STEPS):
        last = step == STEPS - 1
        lon = swap(messages[:2], "lon")
        mid = swap((mid0, mid1), "lon")
        lat = swap(messages[2:], "lat")
        if step == 0:
            weights = hold(tiles.reshape(clusters, slots * nodes, nodes))
        ends = call(corner_kernel, [block(2)] * 2, lon)
        ends = swap(ends, "lat")
        main = functools.partial(main_kernel, shape, slots, last, scale)
        tail = functools.partial(tail_kernel, shape, slots, last, scale)
        given = [idx, state, *lon, *mid, *lat, weights, tot]
        if last:
            ends_at = corner_places(shape)
            few = len(ends_at)
            outs = [((clusters, nodes, dests), bf), ((columns, rows, nodes), f32), block(depth)]
            scratch = [VMEM((clusters - few, nodes, dests), bf), pltpu.SemaphoreType.DMA((clusters - few,))]
            visits, grad, pool = call(main, outs, [*given, demo], work * 3 // 4, scratch, plain=(0,))
            grad, _, turned = call(
                tail,
                [*outs[1:], ((few, nodes, dests), bf)],
                [idx, *ends, weights, tot, grad, pool, demo],
                work // 4,
                same={5: 0, 6: 1},
            )
            (visits,) = call(
                functools.partial(flush_kernel, ends_at),
                outs[:1],
                [turned, visits],
                1 << 22,
                [pltpu.SemaphoreType.DMA((few,))],
                same={1: 0},
                plain=(0,),
            )
        else:
            outs = [block(clusters), sums, block(depth)]
            new, tot_new, pool, mid0, mid1 = call(main, outs + middle, given, work * 3 // 4)
            state, tot, _, *messages = call(
                tail, outs + edges, [idx, *ends, weights, tot, new, tot_new, pool], work // 4, same={5: 0, 6: 1, 7: 2}
            )
    if lax.axis_size("dest") == 2:
        grad = grad + lax.ppermute(grad, "dest", [(0, 1), (1, 0)])
    else:
        grad = lax.psum(grad, "dest")
    return visits.reshape(start_visits.shape), grad


def solution(mesh):
    return jax.shard_map(
        on_device,
        mesh=mesh,
        in_specs=(
            P("lon", "lat", None, "dest"),
            P("lon", "lat", None, None, None),
            P("lon", "lat", None),
            P("lon", "lat"),
            P("lon", "lat", "dest"),
        ),
        out_specs=(P("lon", "lat", None, "dest"), P("lon", "lat", None)),
        check_vma=False,
    )
```
